32 devices in a mesh: dp: 4 (over x, core), expert: 8 (over z, y).
Axes of the slice: x: 2, y: 2, z: 4, core: 2. Of those that a mesh axis runs over, the one named last changes fastest.
Arguments:
- tokens: bfloat16 [32768, 768], P(('dp', 'expert')), may hold values from -6 to 6
- segment: int32 [32768], P(('dp', 'expert')), may hold values from 0 to 15, as said below
- valid: int32 [32768], P(('dp', 'expert')), may hold values from 0 to 1, as said below
- routes: int32 [32768, 2], P(('dp', 'expert')), may hold values from 0 to 31, all different within a row
- out_grad: bfloat16 [32768, 768], P(('dp', 'expert')), may hold values from -6 to 6
- norm1_gain: float32 [768], P(('dp', 'expert')), may hold values from 0.5 to 1.5
- qkv_weight: float32 [2304, 768], P(('dp', 'expert')), may hold values from -0.21875 to 0.21875
- out_weight: float32 [768, 768], P(('dp', 'expert')), may hold values from -0.875 to 0.875
- norm2_gain: float32 [768], P(('dp', 'expert')), may hold values from 0.5 to 1.5
- router: float32 [768, 32], P(('dp', 'expert')), may hold values from -0.15625 to 0.15625
- train_in: float32 [16, 768, 3072], P('expert', None, 'dp'), may hold values from -0.21875 to 0.21875
- train_out: float32 [16, 768, 3072], P('expert', None, 'dp'), may hold values from -0.15625 to 0.15625
- frozen_in: float32 [16, 768, 3072], P('expert', None, 'dp'), may hold values from -0.21875 to 0.21875
- frozen_out: float32 [16, 768, 3072], P('expert', None, 'dp'), may hold values from -0.15625 to 0.15625
Outputs:
- output: bfloat16 [32768, 768], P(('dp', 'expert'))
- tokens_grad: bfloat16 [32768, 768], P(('dp', 'expert'))
- norm1_gain_grad: float32 [768], P(('dp', 'expert'))
- qkv_weight_grad: float32 [2304, 768], P(('dp', 'expert'))
- out_weight_grad: float32 [768, 768], P(('dp', 'expert'))
- norm2_gain_grad: float32 [768], P(('dp', 'expert'))
- router_grad: float32 [768, 32], P(('dp', 'expert'))
- train_in_grad: float32 [16, 768, 3072], P('expert', None, 'dp')
- train_out_grad: float32 [16, 768, 3072], P('expert', None, 'dp')
The draws below stay inside these ranges and needn't reach their ends.
Inputs may be any that keep to these rules, and one draw needn't show every extreme that they name: `segment`: within each pack of 1024 consecutive tokens the sequence numbers start at 0, never fall and rise by one at each new sequence; every sequence fills a whole multiple of 64 tokens; in every draw some pack holds a single sequence and another holds only sequences of 64 tokens. `valid`: in each sequence the tokens are 1 except its last 0 to 31 tokens, which are 0. `routes`: the two experts of a row differ.
All inputs are finite; a program needn't handle non-finite values.
Results may differ from the reference program's by a relative error of at most 0.014.
Values may be sent and summed in bfloat16 or wider, within the bound.
A program may use at most 320 MiB of HBM per device.

```python
from functools import partial
import jax
import jax.numpy as jnp
from jax import lax

D = 768
H = 12
HD = 64
FF = 3072
E = 32
ET = 16
TOK_DEV = 1024
SEG_MIN = 64
CAP = 96
PACKS = 32
TOKENS = 32768


def pack_layout(key):
    blocks = TOK_DEV // SEG_MIN
    kind_key, start_key, whole_key, pad_key = jax.random.split(jax.random.fold_in(key, 11), 4)
    kind = jax.random.randint(kind_key, (PACKS, 1), 0, 3)
    limit = jnp.where(kind == 0, 8, jnp.where(kind == 1, 30, 60))
    drawn_start = jax.random.randint(start_key, (PACKS, blocks), 0, 100) < limit
    first_block = jnp.arange(blocks)[None, :] == 0
    whole_pack = jax.random.randint(whole_key, (), 0, PACKS)
    short_pack = (whole_pack + 1) % PACKS
    pack_rows = jnp.arange(PACKS)[:, None]
    starts = jnp.where(pack_rows == whole_pack, first_block, drawn_start | first_block)
    starts = jnp.where(pack_rows == short_pack, jnp.ones_like(starts), starts)
    seg_blocks = jnp.cumsum(starts.astype(jnp.int32), axis=1, dtype=jnp.int32) - 1
    last_block = jnp.concatenate([starts[:, 1:], jnp.ones((PACKS, 1), dtype=bool)], axis=1)
    pads = jax.random.randint(pad_key, (PACKS, blocks), 0, SEG_MIN // 2)
    kept_rows = jnp.where(last_block, SEG_MIN - pads, SEG_MIN)
    offsets = jnp.arange(SEG_MIN, dtype=jnp.int32)[None, None, :]
    live_rows = (offsets < kept_rows[:, :, None]).astype(jnp.int32)
    seg_rows = jnp.repeat(seg_blocks, SEG_MIN, axis=1).astype(jnp.int32)
    return (seg_rows.reshape(-1), live_rows.reshape(-1))


def draw_segment(key, part):
    return pack_layout(key)[0]


def draw_valid(key, part):
    return pack_layout(key)[1]


def with_spikes(result, rng, source, target, parts, factor):
    owner, partner = [(jnp.arange(result.shape[position]) // (result.shape[position] // parts)).reshape([-1 if axis == position else 1 for axis in range(result.ndim)]) for position in (source, target)]
    chosen = jax.random.permutation(rng, parts)[partner]
    strong = (owner == chosen) | (owner == (partner + parts // 2) % parts)
    return jnp.where(strong, factor * result, result)


def levels(rng, extent, shards, low, largest):
    level = 1.0
    for position, blocks in shards:
        steps = jax.random.uniform(jax.random.fold_in(jax.random.fold_in(rng, 6), position), (blocks,), jnp.float32, low / len(shards), largest / len(shards))
        level = level * jnp.repeat(jnp.exp(steps), extent[position] // blocks).reshape((-1,) + (1,) * (len(extent) - 1 - position))
    return level


def picks_of(rng, rows, amount, top, lift):
    ranking = jax.random.permutation(jax.random.fold_in(rng, 1), amount)
    favour = ranking
    for power in range(3):
        favour = favour * favour // amount
    favour = favour * lift // amount
    chance = jax.random.randint(jax.random.fold_in(rng, 2), (rows, amount), 0, 4096) + favour
    holders = jax.random.permutation(jax.random.fold_in(rng, 3), rows)[jnp.arange(amount) % rows]
    chance = jnp.where(jnp.arange(rows)[:, None] == holders[None, :], 1 << 14, chance)
    merit = chance * amount + jnp.arange(amount)
    return lax.top_k(merit.astype(jnp.int32), top)[1].astype(jnp.int32)


def scatter_about(own_key, shape, scale, bound, cuts=(), held_as=jnp.bfloat16):
    drawn = jax.random.normal(own_key, shape, jnp.float32) * scale
    if len(cuts) > 0:
        drawn = levels(own_key, shape, cuts, -0.22, 0.18) * drawn
    return jnp.clip(drawn, min=-bound, max=bound).astype(held_as)


def heavy_noise(rng, dims, width, most, cuts, heavy, held_as=jnp.bfloat16):
    result = width * jax.random.normal(rng, dims, jnp.float32)
    if cuts:
        result = result * levels(rng, dims, cuts, -0.22, 0.18)
    return jnp.clip(with_spikes(result, jax.random.fold_in(rng, 3), *heavy), -most, most).astype(held_as)


def setup_inputs(seed: int = 0) -> dict:
    keys = jax.random.split(jax.random.key(seed), 15)
    tokens = scatter_about(keys[0], (TOKENS, D), 1.0, 6.0, ((0, 32),))
    segment = draw_segment(jax.random.fold_in(keys[14], 71), 0)
    valid = draw_valid(jax.random.fold_in(keys[14], 71), 0)
    routes = picks_of(keys[3], TOKENS, E, 2, 512)
    out_grad = heavy_noise(keys[4], (TOKENS, D), 1.0, 6.0, ((0, 32),), (0, 1, 32, 2.75))
    norm1_gain = jnp.clip(1.0 + 0.1 * jax.random.normal(keys[5], (D,), jnp.float32), 0.5, 1.5)
    qkv_weight = scatter_about(keys[6], (3 * D, D), D ** -0.5, 0.21875, ((0, 32),), jnp.float32)
    out_weight = scatter_about(keys[7], (D, D), (D // 16) ** -0.5, 0.875, ((0, 32),), jnp.float32)
    norm2_gain = jnp.clip(1.0 + 0.1 * jax.random.normal(keys[8], (D,), jnp.float32), 0.5, 1.5)
    router = scatter_about(keys[9], (D, E), (2 * D) ** -0.5, 0.15625, ((0, 32),), jnp.float32)
    train_in = scatter_about(keys[10], (ET, D, FF), D ** -0.5, 0.21875, ((0, 8), (2, 4)), jnp.float32)
    train_out = scatter_about(keys[11], (ET, D, FF), (FF // 2) ** -0.5, 0.15625, ((0, 8), (2, 4)), jnp.float32)
    frozen_in = scatter_about(keys[12], (ET, D, FF), D ** -0.5, 0.21875, ((0, 8), (2, 4)), jnp.float32)
    frozen_out = scatter_about(keys[13], (ET, D, FF), (FF // 2) ** -0.5, 0.15625, ((0, 8), (2, 4)), jnp.float32)
    return dict(tokens=tokens, segment=segment, valid=valid, routes=routes, out_grad=out_grad, norm1_gain=norm1_gain, qkv_weight=qkv_weight, out_weight=out_weight, norm2_gain=norm2_gain, router=router, train_in=train_in, train_out=train_out, frozen_in=frozen_in, frozen_out=frozen_out)


@jax.custom_vjp
def low(v):
    return lax.optimization_barrier(v.astype(jnp.bfloat16)).astype(jnp.float32)

@jax.custom_vjp
def low_back(v):
    return v

def low_keep(v):
    return (low(v), None)

def low_pass(kept, grad):
    return (grad,)

def back_keep(v):
    return (v, None)

def back_low(kept, grad):
    return (low(grad),)
low.defvjp(low_keep, low_pass)
low_back.defvjp(back_keep, back_low)
epsilon = 1e-05
masked_score = -1e+30
highest = lax.Precision.HIGHEST

def layer_norm(values):
    centre = lax.optimization_barrier(jnp.mean(values, axis=-1, keepdims=True))
    centred = values - centre
    spread = lax.optimization_barrier(jnp.mean(centred * centred, axis=-1, keepdims=True))
    return centred * lax.rsqrt(spread + epsilon)

def gelu_tanh(values):
    return jax.nn.gelu(values, approximate=True)

def slot_table(route_ids, valid_ids, expert_count, capacity):
    pair_ids = route_ids.reshape(-1)
    pair_live = jnp.repeat(valid_ids, 2) > 0
    onehot = ((pair_ids[:, None] == jnp.arange(expert_count, dtype=jnp.int32)[None, :]) & pair_live[:, None]).astype(jnp.int32)
    earlier = jnp.cumsum(onehot, axis=0, dtype=jnp.int32) - onehot
    slot_ids = lax.optimization_barrier(jnp.sum(earlier * onehot, axis=1, dtype=jnp.int32))
    kept = pair_live & (slot_ids < capacity)
    return (slot_ids.reshape(-1, 2), kept.reshape(-1, 2))

def pack_attention(inputs):
    query, key_rows, value_rows, seg_ids, valid_ids = inputs
    row_count = query.shape[0]
    query_head = query.reshape(row_count, H, HD)
    key_head = key_rows.reshape(row_count, H, HD)
    value_head = value_rows.reshape(row_count, H, HD)
    scores = jnp.einsum('qhd,khd->hqk', query_head, key_head, precision=highest) * HD ** (-0.5)
    scores = low_back(scores)
    positions = jnp.arange(row_count, dtype=jnp.int32)
    seen_pairs = (seg_ids[:, None] == seg_ids[None, :]) & (positions[None, :] <= positions[:, None]) & (valid_ids[None, :] > 0)
    scores = jnp.where(seen_pairs[None], scores, masked_score)
    attention = low(jax.nn.softmax(scores, axis=-1))
    combined = jnp.einsum('hqk,khd->qhd', attention, value_head, precision=highest)
    return low_back(low(combined.reshape(row_count, H * HD)))

def expert_apply(inputs):
    row_data, weight_in, weight_out = inputs
    inner = low_back(jnp.dot(row_data, weight_in, precision=highest))
    active = low(gelu_tanh(inner))
    return low_back(low(jnp.dot(active, weight_out.T, precision=highest)))

def reference(tokens, segment, valid, routes, out_grad, norm1_gain, qkv_weight, out_weight, norm2_gain, router, train_in, train_out, frozen_in, frozen_out):
    slot_ids, kept = jax.vmap(partial(slot_table, expert_count=E, capacity=CAP))(routes.reshape(PACKS, TOK_DEV, 2), valid.reshape(PACKS, TOK_DEV))
    slot_ids = slot_ids.reshape(TOKENS, 2)
    kept = kept.reshape(TOKENS, 2)
    pack_ids = (jnp.arange(TOKENS, dtype=jnp.int32) // TOK_DEV)[:, None]
    buffer_rows = PACKS * CAP
    dest = jnp.where(kept, routes * buffer_rows + pack_ids * CAP + slot_ids, E * buffer_rows).astype(jnp.int32)
    valid_f = valid.astype(jnp.float32)[:, None]
    kept_f = kept.astype(jnp.float32)
    frozen_in_low = low(frozen_in)
    frozen_out_low = low(frozen_out)
    choose = (routes[:, :, None] == jnp.arange(E, dtype=jnp.int32)[None, None, :]).astype(jnp.float32)

    def forward(tokens_f, gain_one, qkv_master, out_master, gain_two, router_master, train_in_master, train_out_master):
        norm_one = layer_norm(tokens_f)
        act = low(norm_one * low(gain_one))
        qkv_low = low(qkv_master)
        query = low_back(low(jnp.dot(act, qkv_low[:D], precision=highest)))
        key_rows = low_back(low(jnp.dot(act, qkv_low[D:2 * D], precision=highest)))
        value_rows = low_back(low(jnp.dot(act, qkv_low[2 * D:], precision=highest)))
        heads_out = lax.map(jax.checkpoint(pack_attention), (query.reshape(PACKS, TOK_DEV, D), key_rows.reshape(PACKS, TOK_DEV, D), value_rows.reshape(PACKS, TOK_DEV, D), segment.reshape(PACKS, TOK_DEV), valid.reshape(PACKS, TOK_DEV)))
        attn = low_back(jnp.dot(heads_out.reshape(TOKENS, D), low(out_master), precision=highest)) * valid_f
        resid = tokens_f + attn
        norm_two = layer_norm(resid)
        hidden = low(norm_two * low(gain_two))
        logits = low_back(jnp.dot(hidden, low(router_master), precision=highest))
        soft = jax.nn.softmax(logits, axis=-1)
        picked = lax.optimization_barrier(jnp.sum(soft[:, None, :] * choose, axis=2))
        gates = picked / lax.optimization_barrier(jnp.sum(picked, axis=1, keepdims=True))
        spread_rows = jnp.zeros((E * buffer_rows + 1, D), jnp.float32).at[dest.reshape(-1)].add(jnp.repeat(hidden, 2, axis=0))
        dispatched = low_back(spread_rows[:-1].reshape(E, buffer_rows, D))
        weight_in = jnp.stack([low(train_in_master), frozen_in_low], axis=1).reshape(E, D, FF)
        weight_out = jnp.stack([low(train_out_master), frozen_out_low], axis=1).reshape(E, D, FF)
        returned = lax.map(jax.checkpoint(expert_apply), (dispatched, weight_in, weight_out))
        padded = jnp.concatenate([returned.reshape(E * buffer_rows, D), jnp.zeros((1, D), jnp.float32)], axis=0)
        chosen = padded[dest]
        mixture = lax.optimization_barrier(jnp.sum(chosen * (gates * kept_f)[:, :, None], axis=1))
        return (resid + mixture) * valid_f
    primal, pull = jax.vjp(forward, tokens.astype(jnp.float32), norm1_gain, qkv_weight, out_weight, norm2_gain, router, train_in, train_out)
    grads = pull(out_grad.astype(jnp.float32))
    return (primal.astype(jnp.bfloat16), grads[0].astype(jnp.bfloat16), grads[1], grads[2], grads[3], grads[4], grads[5], grads[6], grads[7])
```

```python
import functools

import jax
import jax.numpy as jnp
from jax import lax
from jax.experimental import pallas as pl
from jax.experimental.pallas import tpu as pltpu
from jax.sharding import PartitionSpec as P

HD = 64
CAP = 96
EXTRA = 16

epsilon = 1e-05
masked_score = -1e30
F32 = jnp.float32
BF = jnp.bfloat16


def layer_norm(values):
    centre = jnp.mean(values, axis=-1, keepdims=True)
    centred = values - centre
    spread = jnp.mean(centred * centred, axis=-1, keepdims=True)
    return centred * lax.rsqrt(spread + epsilon)


def seen_pairs(seg_ids, valid_ids, row_start, row_stop):
    rows_here = jnp.arange(row_start, row_stop, dtype=jnp.int32)[:, None]
    keys_here = jnp.arange(row_stop, dtype=jnp.int32)[None, :]
    same_segment = seg_ids[row_start:row_stop, None] == seg_ids[None, :row_stop]
    return same_segment & (keys_here <= rows_here) & (valid_ids[None, :row_stop] > 0)


def attend_forward(query, key_rows, value_rows, seg_ids, valid_ids, head_count):
    row_count = query.shape[0]
    block_rows = min(512, row_count)
    scale = HD ** (-0.5)
    out_blocks = []
    log_sums = []
    for row_start in range(0, row_count, block_rows):
        row_stop = row_start + block_rows
        query_head = query[row_start:row_stop].reshape(block_rows, head_count, HD)
        key_head = key_rows[:row_stop].reshape(row_stop, head_count, HD)
        value_head = value_rows[:row_stop].reshape(row_stop, head_count, HD)
        scores = (
            jnp.einsum("qhd,khd->hqk", query_head, key_head, preferred_element_type=jnp.float32)
            * scale
        )
        scores = jnp.where(
            seen_pairs(seg_ids, valid_ids, row_start, row_stop)[None], scores, masked_score
        )
        row_max = jnp.max(scores, axis=-1, keepdims=True)
        exponent = jnp.exp(scores - row_max)
        row_total = jnp.sum(exponent, axis=-1, keepdims=True)
        attention = (exponent / row_total).astype(jnp.bfloat16)
        combined = jnp.einsum(
            "hqk,khd->qhd", attention, value_head, preferred_element_type=jnp.float32
        )
        out_blocks.append(combined.reshape(block_rows, head_count * HD).astype(jnp.bfloat16))
        log_sums.append(row_max + jnp.log(row_total))
    return (jnp.concatenate(out_blocks, axis=0), log_sums)


def attend_backward(query, key_rows, value_rows, d_heads, seg_ids, valid_ids, log_sums, head_count):
    row_count = query.shape[0]
    block_rows = min(512, row_count)
    scale = HD ** (-0.5)
    d_query_blocks = []
    d_key = jnp.zeros((row_count, head_count, HD), jnp.float32)
    d_value = jnp.zeros((row_count, head_count, HD), jnp.float32)
    for block_number, row_start in enumerate(range(0, row_count, block_rows)):
        row_stop = row_start + block_rows
        query_head = query[row_start:row_stop].reshape(block_rows, head_count, HD)
        key_head = key_rows[:row_stop].reshape(row_stop, head_count, HD)
        value_head = value_rows[:row_stop].reshape(row_stop, head_count, HD)
        grad_head = d_heads[row_start:row_stop].reshape(block_rows, head_count, HD)
        scores = (
            jnp.einsum("qhd,khd->hqk", query_head, key_head, preferred_element_type=jnp.float32)
            * scale
        )
        scores = jnp.where(
            seen_pairs(seg_ids, valid_ids, row_start, row_stop)[None], scores, masked_score
        )
        attention = jnp.exp(scores - log_sums[block_number])
        d_attention = jnp.einsum(
            "qhd,khd->hqk", grad_head, value_head, preferred_element_type=jnp.float32
        )
        d_scores = (
            attention * (d_attention - jnp.sum(d_attention * attention, axis=-1, keepdims=True))
        ).astype(jnp.bfloat16)
        d_query_blocks.append(
            (
                jnp.einsum("hqk,khd->qhd", d_scores, key_head, preferred_element_type=jnp.float32)
                * scale
            ).reshape(block_rows, head_count * HD)
        )
        d_key = d_key.at[:row_stop].add(
            jnp.einsum("hqk,qhd->khd", d_scores, query_head, preferred_element_type=jnp.float32)
            * scale
        )
        d_value = d_value.at[:row_stop].add(
            jnp.einsum(
                "hqk,qhd->khd",
                attention.astype(jnp.bfloat16),
                grad_head,
                preferred_element_type=jnp.float32,
            )
        )
    d_query = jnp.concatenate(d_query_blocks, axis=0).astype(jnp.bfloat16)
    return (
        d_query,
        d_key.reshape(row_count, head_count * HD).astype(jnp.bfloat16),
        d_value.reshape(row_count, head_count * HD).astype(jnp.bfloat16),
    )


def iota(shape, axis):
    return lax.broadcasted_iota(jnp.int32, shape, axis)


def dot(a, b):
    return jnp.dot(a, b, preferred_element_type=F32)


def dot_nt(a, b):
    return lax.dot_general(a, b, (((1,), (1,)), ((), ())), preferred_element_type=F32)


def lanes_up(count):
    return -(-count // 128) * 128


def cost(flops, nbytes):
    return pl.CostEstimate(flops=int(flops), bytes_accessed=int(nbytes), transcendentals=0)


def whole(shape):
    zeros = (0,) * len(shape)
    return pl.BlockSpec(shape, lambda *_: zeros)


def dispatch_rows(group, slot_ref, rows_ref, a_ref, b_ref, local_count):
    half = local_count // 2
    tokens = rows_ref.shape[0]
    slots = iota((CAP, tokens), 0)
    picks = []
    for c in range(2):
        for i in range(half):
            row = slot_ref[pl.ds(group * local_count + 2 * i + c, 1), :]
            picks.append((row == slots).astype(F32).astype(BF))
    chosen = jnp.concatenate(picks, axis=0)
    moved = dot(chosen, rows_ref[...]).astype(BF)
    a_ref[0, : half * CAP, :] = moved[: half * CAP]
    b_ref[0, : half * CAP, :] = moved[half * CAP :]
    return chosen


def first_dispatch_kernel(
    routes_ref, routes_t_ref, valid_ref, valid_t_ref, rows_ref,
    slot_ref, dest_ref, a_ref, b_ref, *, expert_count, local_count,
):
    group = pl.program_id(0)
    tokens = rows_ref.shape[0]
    half = local_count // 2

    @pl.when(group == 0)
    def _():
        row_ids = iota((tokens, tokens), 0)
        col_ids = iota((tokens, tokens), 1)
        experts_t = iota((expert_count, tokens), 0)
        live_t = (
            (routes_t_ref[0:1, :] == experts_t) | (routes_t_ref[1:2, :] == experts_t)
        ) & (valid_t_ref[...] > 0)
        above = (row_ids < col_ids).astype(F32).astype(BF)
        earlier_t = dot(live_t.astype(F32).astype(BF), above)
        slot_ref[...] = jnp.where(
            live_t & (earlier_t < CAP), earlier_t, -1.0
        ).astype(jnp.int32)

        experts = iota((tokens, expert_count), 1)
        first = routes_ref[:, 0:1]
        second = routes_ref[:, 1:2]
        live = ((first == experts) | (second == experts)) & (valid_ref[...] > 0)
        below = (col_ids < row_ids).astype(F32).astype(BF)
        earlier = dot(below, live.astype(F32).astype(BF))
        kept = jnp.where(live & (earlier < CAP), earlier, -1.0)
        lanes = iota((tokens, 128), 1)
        table = jnp.full((tokens, 128), -1, jnp.int32)
        bits = local_count.bit_length() - 1
        for k, route in enumerate((first, second)):
            slot = jnp.sum(
                jnp.where(route == experts, kept, 0.0), axis=1, keepdims=True
            ).astype(jnp.int32)
            place = lax.shift_right_logical(route, bits)
            inner = lax.shift_right_logical(route & (local_count - 1), 1)
            for stride, base in ((half * CAP + EXTRA, 0), (half * CAP, 4)):
                code = place * stride + inner * CAP + slot
                for c in range(2):
                    ok = (slot >= 0) & ((route & 1) == c)
                    table = jnp.where(
                        lanes == base + 2 * c + k, jnp.where(ok, code, -1), table
                    )
        dest_ref[...] = table

    dispatch_rows(group, slot_ref, rows_ref, a_ref, b_ref, local_count)


def first_dispatch(routes, valid, rows, expert_count, groups):
    tokens, width = rows.shape
    local_count = expert_count // groups
    block = (local_count // 2) * CAP
    out_spec = pl.BlockSpec((1, block, width), lambda g: (g, 0, 0))
    return pl.pallas_call(
        functools.partial(
            first_dispatch_kernel, expert_count=expert_count, local_count=local_count
        ),
        name="first_dispatch",
        grid=(groups,),
        in_specs=[
            whole((tokens, 2)), whole((2, tokens)), whole((tokens, 1)), whole((1, tokens)),
            whole((tokens, width)),
        ],
        out_specs=[whole((expert_count, tokens)), whole((tokens, 128)), out_spec, out_spec],
        out_shape=[
            jax.ShapeDtypeStruct((expert_count, tokens), jnp.int32),
            jax.ShapeDtypeStruct((tokens, 128), jnp.int32),
            jax.ShapeDtypeStruct((groups, block, width), BF),
            jax.ShapeDtypeStruct((groups, block, width), BF),
        ],
        cost_estimate=cost(2 * expert_count * CAP * tokens * width, 8e6),
    )(routes, routes.T, valid[:, None], valid[None, :], rows)


def split_two(values):
    high = values.astype(BF).astype(F32)
    return high, values - high


def second_dispatch_kernel(slot_ref, gate_ref, rows_ref, a_ref, b_ref, *, local_count):
    group = pl.program_id(0)
    half = local_count // 2
    total = local_count * CAP
    block = half * CAP
    width = rows_ref.shape[1]
    chosen = dispatch_rows(group, slot_ref, rows_ref, a_ref, b_ref, local_count)
    high, low = split_two(gate_ref[...])
    experts = gate_ref.shape[0]
    every = dot_nt(jnp.concatenate([high.astype(BF), low.astype(BF)], axis=0), chosen)
    column = iota((experts, total), 1)
    expert = iota((experts, total), 0)
    mine = jnp.zeros((experts, total), jnp.bool_)
    for c in range(2):
        for i in range(half):
            start = (c * half + i) * CAP
            mine = mine | (
                (column >= start)
                & (column < start + CAP)
                & (expert == group * local_count + 2 * i + c)
            )
    high_row = jnp.sum(jnp.where(mine, every[:experts], 0.0), axis=0, keepdims=True)
    low_row = jnp.sum(jnp.where(mine, every[experts:], 0.0), axis=0, keepdims=True)
    sub = iota((EXTRA, total), 0)
    tail = jnp.where(sub == 0, high_row, jnp.where(sub == 1, low_row, 0.0)).astype(BF)
    for ref in (a_ref, b_ref):
        ref[0, block:, :] = jnp.zeros((EXTRA, width), BF)
        ref[0, block:, :total] = tail


def second_dispatch(slot_table, gate_t, rows, groups):
    tokens, width = rows.shape
    expert_count = slot_table.shape[0]
    local_count = expert_count // groups
    block = (local_count // 2) * CAP + EXTRA
    out_spec = pl.BlockSpec((1, block, width), lambda g: (g, 0, 0))
    return pl.pallas_call(
        functools.partial(second_dispatch_kernel, local_count=local_count),
        name="second_dispatch",
        grid=(groups,),
        in_specs=[
            whole((expert_count, tokens)), whole((expert_count, tokens)), whole((tokens, width)),
        ],
        out_specs=[out_spec, out_spec],
        out_shape=[jax.ShapeDtypeStruct((groups, block, width), BF)] * 2,
        cost_estimate=cost(2 * expert_count * CAP * tokens * width, 8e6),
    )(slot_table, gate_t, rows)


GELU_SLOPE = 0.7978845608028654
GELU_CUBE = 0.044715


def expert_kernel(*refs, train, chunk, half, groups, row_block):
    if train:
        x_ref, t_ref, u_ref, v_ref, y_ref, dx_ref, gu_ref, gv_ref = refs[:8]
        xs, dys, gate_s, y_acc, dx_acc, c_s, dz_s, x_t, dy_t = refs[8:]
    else:
        x_ref, t_ref, u_ref, v_ref, y_ref, dx_ref = refs[:6]
        xs, dys, gate_s, y_acc, dx_acc = refs[6:]
    i = pl.program_id(0)
    f = pl.program_id(1)
    block = half * CAP
    width = xs.shape[1]
    rows = groups * CAP
    mine = pl.ds(pl.multiple_of(i * CAP, CAP), CAP)

    @pl.when((i == 0) & (f == 0))
    def _():
        dx_ref[:, block:, :] = jnp.zeros((groups, EXTRA, width), BF)

    @pl.when(f == 0)
    def _():
        wide = lanes_up(2 * block)
        lane = iota((CAP, wide), 1)
        sub = iota((CAP, wide), 0)
        hit = lane == sub + (chunk * half + i) * CAP
        for g in range(groups):
            at = slice(g * CAP, (g + 1) * CAP)
            gates = jnp.sum(
                x_ref[g, block:, :wide].astype(F32), axis=0, keepdims=True
            )
            gate = jnp.sum(jnp.where(hit, gates, 0.0), axis=1, keepdims=True)
            gate_s[at, :] = jnp.broadcast_to(gate, (CAP, 128))
            x = x_ref[g, mine, :]
            xs[at, :] = x
            dy = (gate * t_ref[g, mine, :].astype(F32)).astype(BF)
            dys[at, :] = dy
        y_acc[...] = jnp.zeros((rows, width), F32)
        dx_acc[...] = jnp.zeros((rows, width), F32)
        if train:
            x_t[...] = xs[...].T
            dy_t[...] = dys[...].T

    @pl.loop(0, rows // row_block)
    def _(b):
        at = pl.ds(pl.multiple_of(b * row_block, row_block), row_block)
        u = u_ref[0, 0]
        v = v_ref[0, 0]
        z = dot(xs[at, :], u)
        dc = dot(dys[at, :], v)
        square = z * z
        bend = jnp.tanh(GELU_SLOPE * z * (1.0 + GELU_CUBE * square))
        half_up = 0.5 + 0.5 * bend
        c = (z * half_up).astype(BF)
        slope = half_up + (0.5 * GELU_SLOPE) * z * (1.0 - bend * bend) * (
            1.0 + (3.0 * GELU_CUBE) * square
        )
        dz = (dc * slope).astype(BF)
        y_acc[at, :] += dot_nt(c, v)
        dx_acc[at, :] += dot_nt(dz, u)
        if train:
            c_s[at, :] = c
            dz_s[at, :] = dz

    if train:
        step = min(256, width)

        @pl.loop(0, width // step)
        def _(b):
            at = pl.ds(pl.multiple_of(b * step, step), step)
            gu_ref[0, 0, at, :] = dot(x_t[at, :], dz_s[...]).astype(BF)
            gv_ref[0, 0, at, :] = dot(dy_t[at, :], c_s[...]).astype(BF)

    @pl.when(f == pl.num_programs(1) - 1)
    def _():
        wide = lanes_up(block)
        lane = iota((CAP, wide), 1)
        sub = iota((CAP, wide), 0)
        hit = lane == sub + i * CAP
        tail_sub = iota((EXTRA, wide), 0)
        for g in range(groups):
            at = slice(g * CAP, (g + 1) * CAP)
            y = y_acc[at, :].astype(BF).astype(F32)
            d_gate = jnp.sum(t_ref[g, mine, :].astype(F32) * y, axis=1, keepdims=True)
            row = jnp.sum(jnp.where(hit, d_gate, 0.0), axis=0, keepdims=True)
            high, low = split_two(row)
            tail = jnp.where(tail_sub == 0, high, jnp.where(tail_sub == 1, low, 0.0))
            dx_ref[g, block:, :wide] = (
                dx_ref[g, block:, :wide].astype(F32) + tail
            ).astype(BF)
            y_ref[g, mine, :] = (gate_s[at, 0:1] * y).astype(BF)
            dx_ref[g, mine, :] = dx_acc[at, :].astype(BF)


def run_experts(x_rows, t_rows, weight_in, weight_out, chunk, train):
    groups, x_block, width = x_rows.shape
    block = x_block - EXTRA
    parts, half, _, hidden = weight_in.shape
    rows = groups * CAP
    weight_spec = pl.BlockSpec((1, 1, width, hidden), lambda i, f: (f, i, 0, 0))
    out_specs = [whole((groups, block, width)), whole((groups, x_block, width))]
    out_shape = [
        jax.ShapeDtypeStruct((groups, block, width), BF),
        jax.ShapeDtypeStruct((groups, x_block, width), BF),
    ]
    scratch = [
        pltpu.VMEM((rows, width), BF), pltpu.VMEM((rows, width), BF),
        pltpu.VMEM((rows, 128), F32),
        pltpu.VMEM((rows, width), F32), pltpu.VMEM((rows, width), F32),
    ]
    if train:
        out_specs += [weight_spec, weight_spec]
        out_shape += [jax.ShapeDtypeStruct(weight_in.shape, BF)] * 2
        scratch += [
            pltpu.VMEM((rows, hidden), BF), pltpu.VMEM((rows, hidden), BF),
            pltpu.VMEM((width, rows), BF), pltpu.VMEM((width, rows), BF),
        ]
    products = 6 if train else 4
    return pl.pallas_call(
        functools.partial(
            expert_kernel, train=train, chunk=chunk, half=half, groups=groups,
            row_block=min(256, rows),
        ),
        name="experts_train" if train else "experts_frozen",
        grid=(half, parts),
        in_specs=[
            whole((groups, x_block, width)), whole((groups, block, width)),
            weight_spec, weight_spec,
        ],
        out_specs=out_specs,
        out_shape=out_shape,
        scratch_shapes=scratch,
        cost_estimate=cost(products * 2 * half * rows * width * hidden * parts, 30e6),
    )(x_rows, t_rows, weight_in, weight_out)


def two_hot(dest, column, count):
    place = iota((dest.shape[0], count), 1)
    hit = (dest[:, column : column + 1] == place) | (dest[:, column + 1 : column + 2] == place)
    return hit.astype(F32).astype(BF)


def combine_back_kernel(dest_ref, a_ref, b_ref, rows_ref, gate_ref, table, *, half, groups):
    stride = half * CAP + EXTRA
    block = half * CAP
    count = groups * stride

    @pl.when(pl.program_id(0) == 0)
    def _():
        wide = lanes_up(block)
        eye = iota((block, wide), 0) == iota((block, wide), 1)
        lane = iota((block, 128), 1)
        inner = iota((block, 128), 0) // CAP if half > 1 else jnp.zeros((block, 128), jnp.int32)
        for c, ref in enumerate((a_ref, b_ref)):
            for g in range(groups):
                tail = ref[g * stride + block : (g + 1) * stride, :wide].astype(F32)
                high = jnp.sum(jnp.where(eye, tail[0:1, :], 0.0), axis=1, keepdims=True)
                low = jnp.sum(jnp.where(eye, tail[1:2, :], 0.0), axis=1, keepdims=True)
                spot = 2 * (g * half + inner) + c
                table[c, g * stride : g * stride + block, :] = jnp.where(
                    lane == spot, high, jnp.where(lane == spot + 64, low, 0.0)
                ).astype(BF)
                table[c, g * stride + block : (g + 1) * stride, :] = jnp.zeros((EXTRA, 128), BF)

    dest = dest_ref[...]
    hot_a = two_hot(dest, 0, count)
    hot_b = two_hot(dest, 2, count)
    rows_ref[...] = dot(hot_a, a_ref[...]) + dot(hot_b, b_ref[...])
    gate_ref[...] = dot(hot_a, table[0]) + dot(hot_b, table[1])


def combine_back(dest, rows_a, rows_b, half, groups):
    tokens = dest.shape[0]
    width = rows_a.shape[-1]
    count = groups * (half * CAP + EXTRA)
    step = min(256, tokens)
    row_spec = pl.BlockSpec((step, width), lambda b: (b, 0))
    lane_spec = pl.BlockSpec((step, 128), lambda b: (b, 0))
    return pl.pallas_call(
        functools.partial(combine_back_kernel, half=half, groups=groups),
        name="combine_back",
        grid=(tokens // step,),
        in_specs=[lane_spec, whole((count, width)), whole((count, width))],
        out_specs=[row_spec, lane_spec],
        out_shape=[
            jax.ShapeDtypeStruct((tokens, width), F32),
            jax.ShapeDtypeStruct((tokens, 128), F32),
        ],
        scratch_shapes=[pltpu.VMEM((2, count, 128), BF)],
        cost_estimate=cost(4 * tokens * count * width, 12e6),
    )(dest, rows_a.reshape(count, width), rows_b.reshape(count, width))


def combine_out_kernel(dest_ref, a_ref, b_ref, resid_ref, valid_ref, out_ref):
    count = a_ref.shape[0]
    dest = dest_ref[...]
    mixed = dot(two_hot(dest, 4, count), a_ref[...]) + dot(two_hot(dest, 6, count), b_ref[...])
    out_ref[...] = ((resid_ref[...] + mixed) * valid_ref[...].astype(F32)).astype(BF)


def combine_out(dest, rows_a, rows_b, resid, valid):
    tokens, width = resid.shape
    count = rows_a.shape[0] * rows_a.shape[1]
    step = min(256, tokens)
    return pl.pallas_call(
        combine_out_kernel,
        name="combine_out",
        grid=(tokens // step,),
        in_specs=[
            pl.BlockSpec((step, 128), lambda b: (b, 0)),
            whole((count, width)), whole((count, width)),
            pl.BlockSpec((step, width), lambda b: (b, 0)),
            pl.BlockSpec((step, 1), lambda b: (b, 0)),
        ],
        out_specs=pl.BlockSpec((step, width), lambda b: (b, 0)),
        out_shape=jax.ShapeDtypeStruct((tokens, width), BF),
        cost_estimate=cost(4 * tokens * count * width, 12e6),
    )(dest, rows_a.reshape(count, width), rows_b.reshape(count, width), resid, valid[:, None])


def pad_to(values, count):
    return jnp.pad(values, [(0, 0)] * (values.ndim - 1) + [(0, count - values.shape[-1])])


def swap(rows):
    return lax.all_to_all(rows, "expert", split_axis=0, concat_axis=0, tiled=True)


BOTH = ("dp", "expert")


def local(
    tokens,
    segment,
    valid,
    routes,
    out_grad,
    norm1_gain,
    qkv_weight,
    out_weight,
    norm2_gain,
    router,
    train_in,
    train_out,
    frozen_in,
    frozen_out,
):
    token_count, width = tokens.shape
    head_count = width // HD
    expert_count = router.shape[1]
    groups = lax.axis_size("expert")
    devices = groups * lax.axis_size("dp")
    local_count = expert_count // groups
    half = local_count // 2

    small = jnp.concatenate([router.reshape(-1), norm1_gain, norm2_gain])
    small_rows = -(-small.shape[0] // width)
    small = pad_to(small[None], small_rows * width).reshape(small_rows, width)
    payload = jnp.concatenate([qkv_weight, out_weight, small], axis=0).astype(BF)
    dense = lax.all_gather(payload, BOTH, axis=0, tiled=False)
    q_rows, o_rows, gain_rows = qkv_weight.shape[0], out_weight.shape[0], norm1_gain.shape[0]
    projection_stack = dense[:, :q_rows].reshape(3, width, width)
    attention_out = dense[:, q_rows : q_rows + o_rows].reshape(width, width)
    tail = dense[:, q_rows + o_rows :].reshape(devices, small_rows * width)
    router_size = gain_rows * expert_count
    router_low = tail[:, :router_size].reshape(width, expert_count)
    gain_one = tail[:, router_size : router_size + gain_rows].reshape(width).astype(F32)
    gain_two = (
        tail[:, router_size + gain_rows : router_size + 2 * gain_rows]
        .reshape(width)
        .astype(F32)
    )

    slot_table, dest, t_send_a, t_send_b = first_dispatch(
        routes, valid, out_grad, expert_count, groups
    )
    t_a = swap(t_send_a)
    t_b = swap(t_send_b)

    experts_low = [
        lax.all_gather(w.astype(BF), "dp", axis=0, tiled=False)
        for w in (train_in, train_out, frozen_in, frozen_out)
    ]

    tokens_f = tokens.astype(F32)
    valid_f = valid.astype(F32)[:, None]
    norm_one = layer_norm(tokens_f)
    act = (norm_one * gain_one).astype(BF)
    projected = jnp.einsum(
        "td,jde->jte", act, projection_stack, preferred_element_type=F32
    ).astype(BF)
    query, key_rows, value_rows = (projected[0], projected[1], projected[2])
    heads_out, log_sums = attend_forward(query, key_rows, value_rows, segment, valid, head_count)
    attn = jnp.dot(heads_out, attention_out, preferred_element_type=F32) * valid_f
    resid = tokens_f + attn
    norm_two = layer_norm(resid)
    hidden = (norm_two * gain_two).astype(BF)
    logits = jnp.dot(hidden, router_low, preferred_element_type=F32)
    soft = jax.nn.softmax(logits, axis=-1)
    expert_ids = jnp.arange(expert_count, dtype=jnp.int32)[None, :]
    choose = ((routes[:, 0:1] == expert_ids) | (routes[:, 1:2] == expert_ids)).astype(F32)
    picked = soft * choose
    picked_total = jnp.sum(picked, axis=1, keepdims=True)
    gates = picked / picked_total

    x_send_a, x_send_b = second_dispatch(slot_table, gates.T, hidden, groups)
    x_a = swap(x_send_a)
    x_b = swap(x_send_b)
    y_a, dx_a, grad_in, grad_out = run_experts(
        x_a, t_a, experts_low[0], experts_low[1], 0, True
    )
    dx_a = swap(dx_a)
    y_b, dx_b = run_experts(x_b, t_b, experts_low[2], experts_low[3], 1, False)
    dx_b = swap(dx_b)
    y_a = swap(y_a)
    y_b = swap(y_b)
    grad_train_in = lax.psum_scatter(grad_in, "dp", scatter_dimension=0, tiled=False).astype(F32)
    grad_train_out = lax.psum_scatter(grad_out, "dp", scatter_dimension=0, tiled=False).astype(
        F32
    )
    output = combine_out(dest, y_a, y_b, resid, valid)

    d_hidden, gate_parts = combine_back(dest, dx_a, dx_b, half, groups)
    cotangent = out_grad.astype(F32) * valid_f
    d_gate = gate_parts[:, :expert_count] + gate_parts[:, 64 : 64 + expert_count]
    d_picked = choose * (d_gate - jnp.sum(d_gate * gates, axis=1, keepdims=True)) / picked_total
    d_logits = (soft * (d_picked - jnp.sum(d_picked * soft, axis=-1, keepdims=True))).astype(BF)
    grad_router = jnp.dot(hidden.T, d_logits, preferred_element_type=F32)
    d_hidden = d_hidden + jnp.dot(d_logits, router_low.T, preferred_element_type=F32)
    grad_gain_two = jnp.sum(d_hidden * norm_two, axis=0)
    norm_two_pull = jax.vjp(layer_norm, resid)[1]
    d_resid = cotangent + norm_two_pull(d_hidden * gain_two)[0]
    d_attn = (d_resid * valid_f).astype(BF)
    grad_attention_out = jnp.dot(heads_out.T, d_attn, preferred_element_type=F32)
    early = jnp.concatenate(
        [
            grad_attention_out.reshape(devices, o_rows, width),
            pad_to(
                jnp.concatenate(
                    [
                        grad_router.reshape(devices, router_size),
                        grad_gain_two.reshape(devices, gain_rows),
                    ],
                    axis=1,
                ),
                small_rows * width,
            ).reshape(devices, small_rows, width),
        ],
        axis=1,
    )
    early = lax.psum_scatter(early, BOTH, scatter_dimension=0, tiled=False)
    d_heads = jnp.dot(d_attn, attention_out.T, preferred_element_type=F32).astype(BF)
    d_query, d_key, d_value = attend_backward(
        query, key_rows, value_rows, d_heads, segment, valid, log_sums, head_count
    )
    d_projected = jnp.stack([d_query, d_key, d_value], axis=0)
    grad_projections = jnp.einsum(
        "td,jte->jde", act, d_projected, preferred_element_type=F32
    ).reshape(devices, q_rows, width)
    d_act = jnp.einsum("jte,jde->td", d_projected, projection_stack, preferred_element_type=F32)
    grad_gain_one = jnp.sum(d_act * norm_one, axis=0)
    late = jnp.concatenate(
        [
            grad_projections,
            pad_to(grad_gain_one.reshape(devices, 1, gain_rows), width),
        ],
        axis=1,
    )
    late = lax.psum_scatter(late, BOTH, scatter_dimension=0, tiled=False)
    norm_one_pull = jax.vjp(layer_norm, tokens_f)[1]
    tokens_grad = (d_resid + norm_one_pull(d_act * gain_one)[0]).astype(BF)
    early_tail = early[o_rows:].reshape(-1)
    return (
        output,
        tokens_grad,
        late[q_rows, :gain_rows],
        late[:q_rows],
        early[:o_rows],
        early_tail[router_size : router_size + gain_rows],
        early_tail[:router_size].reshape(gain_rows, expert_count),
        grad_train_in,
        grad_train_out,
    )


def solution(mesh):
    rows = P(("dp", "expert"), None)
    flat = P(("dp", "expert"))
    expert = P("expert", None, "dp")
    return jax.shard_map(
        local,
        mesh=mesh,
        in_specs=(
            rows, flat, flat, rows, rows, flat, rows, rows, flat, rows,
            expert, expert, expert, expert,
        ),
        out_specs=(rows, rows, flat, rows, rows, flat, rows, expert, expert),
        check_vma=False,
    )
```
